256 devices in a mesh: shard: 64 (over z, y, core), col: 4 (over x).
Axes of the slice: x: 4, y: 4, z: 8, core: 2. Of those that a mesh axis runs over, the one named last changes fastest.
Arguments:
- values: float32 [32768, 512], P('shard', 'col'), may hold values from -6 to 6
- keep_mask: int32 [32768], P(('shard', 'col')), may hold values from 0 to 1, as said below
- row_counts: int32 [64], P('shard'), may hold values from 128 to 512
Outputs:
- packed: float32 [32768, 512], P('shard', 'col')
- span_stats: float32 [4, 64, 512], P(None, 'shard', 'col')
The draws below stay inside these ranges and needn't reach their ends.
Inputs may be any that keep to these rules, and one draw needn't show every extreme that they name: `keep_mask`: mostly survivors, with delete-range gaps of 1 to 32 rows, denser in some regions.
All inputs are finite; a program needn't handle non-finite values.
Results may differ from the reference program's by a relative error of at most 0.00002.
Values sent between devices are 32-bit elements; how exact they have to be, the bound alone decides.
A program may use at most 128 MiB of HBM per device.

```python
import jax
import jax.numpy as jnp

CH = 512
COLS = 512
ROWS = 32768
N_SHARD = 64


def draw_store(key):
    counts_key = jax.random.fold_in(key, 7)
    mask_key = jax.random.fold_in(key, 11)
    counts = jax.random.randint(counts_key, (N_SHARD,), CH // 4, CH + 1).astype(jnp.int32)
    first, second, third, fourth = jax.random.split(mask_key, 4)
    ranges = ROWS // 32
    hot_start = jax.random.randint(first, (), 0, N_SHARD) * CH
    spread_starts = jax.random.randint(second, (ranges,), 0, ROWS)
    hot_starts = (hot_start + jax.random.randint(third, (ranges,), 0, 4 * CH)) % ROWS
    starts = jnp.where(jnp.arange(ranges) < ranges // 2, spread_starts, hot_starts)
    lengths = jax.random.randint(fourth, (ranges,), 1, 33)
    ends = jnp.minimum(starts + lengths, ROWS)
    marks = jnp.zeros((ROWS + 1,), jnp.int32).at[starts].add(1).at[ends].add(-1)
    covered = jnp.cumsum(marks)[:ROWS]
    mask = (covered == 0).astype(jnp.int32).reshape(N_SHARD, CH)
    local = jnp.arange(CH, dtype=jnp.int32)[None, :]
    live = mask * (local < counts[:, None]).astype(jnp.int32)
    kept = jnp.sum(live, axis=1)
    wrong = kept % 2 != jnp.arange(N_SHARD, dtype=jnp.int32) % 2
    first_col = jnp.where(wrong, 1 - mask[:, 0], mask[:, 0])
    mask = mask.at[:, 0].set(first_col)
    return (mask.reshape(ROWS).astype(jnp.int32), counts)


def draw_keep_mask(key, part):
    return draw_store(key)[0]


def draw_row_counts(key, part):
    return draw_store(key)[1]


def steps_of(own_key, extent, cuts, smallest, top_value):
    gain, own = 1.0, jax.random.fold_in(own_key, 6)
    for dim, parts in cuts:
        heights = jnp.exp(jax.random.uniform(jax.random.fold_in(own, dim), (parts,), jnp.float32, smallest / len(cuts), top_value / len(cuts)))
        gain = gain * jnp.repeat(heights, extent[dim] // parts).reshape([-1 if axis == dim else 1 for axis in range(len(extent))])
    return gain


def gaussian(stream_key, shape, width, most, shards=(), held_as=jnp.bfloat16):
    array = width * jax.random.normal(stream_key, shape, jnp.float32)
    if shards:
        array = array * steps_of(stream_key, shape, shards, -0.22, 0.18)
    return jnp.clip(array, -most, most).astype(held_as)


def setup_inputs(seed: int = 0) -> dict:
    key_of = jax.random.split(jax.random.key(seed), 4)
    values = gaussian(key_of[0], (ROWS, COLS), 1.0, 6.0, ((0, 64), (1, 4)), jnp.float32)
    keep_mask = draw_keep_mask(jax.random.fold_in(key_of[3], 71), 0)
    row_counts = draw_row_counts(jax.random.fold_in(key_of[3], 71), 0)
    return dict(values=values, keep_mask=keep_mask, row_counts=row_counts)


def reference(values, keep_mask, row_counts):
    rows_all = values.shape[0]
    index = jnp.arange(rows_all, dtype=jnp.int32)
    owner = (index // CH).astype(jnp.int32)
    local = index - owner * CH
    live = (keep_mask == 1) & (local < row_counts[owner])
    live_int = live.astype(jnp.int32)
    before = (jnp.cumsum(live_int) - live_int).astype(jnp.int32)
    total = jnp.sum(live_int).astype(jnp.int32)
    start = (rows_all - total).astype(jnp.int32)
    target = jnp.where(live, start + before, rows_all).astype(jnp.int32)
    packed = jnp.zeros_like(values).at[target].set(values, mode="drop")
    spans = packed.reshape(N_SHARD, CH, values.shape[1])
    ends = (jnp.arange(N_SHARD, dtype=jnp.int32) + 1) * CH
    filled = jnp.clip(ends - start, 0, CH)
    row_live = jnp.arange(CH, dtype=jnp.int32)[None, :] >= (CH - filled)[:, None]
    denom = jnp.maximum(filled.astype(jnp.float32), 1.0)[:, None]
    mean = jnp.sum(spans, axis=1) / denom
    spread = jnp.where(row_live[:, :, None], (spans - mean[:, None, :]) ** 2, 0.0)
    variance = jnp.sum(spread, axis=1) / denom
    has_rows = (filled > 0)[:, None]
    low = jnp.where(has_rows, jnp.min(jnp.where(row_live[:, :, None], spans, jnp.inf), axis=1), 0.0)
    high = jnp.where(has_rows, jnp.max(jnp.where(row_live[:, :, None], spans, -jnp.inf), axis=1), 0.0)
    span_stats = jnp.stack([mean, variance, low, high]).astype(jnp.float32)
    return packed, span_stats
```

```python
import jax
import jax.numpy as jnp
from jax import lax
from jax.sharding import PartitionSpec as P


def gather_directly(value, axis):
    copies = jnp.broadcast_to(value, (lax.axis_size(axis), *value.shape))
    return lax.all_to_all(copies, axis, split_axis=0, concat_axis=0, tiled=True)


def on_device(values, keep_mask, row_counts):
    rows, width = values.shape
    shards = lax.axis_size("shard")
    tile = rows // shards
    me = lax.axis_index("shard")
    mask = gather_directly(keep_mask, "col").reshape(rows)
    local = jnp.arange(rows, dtype=jnp.int32)
    live = (mask == 1) & (local < row_counts[0])
    live_int = live.astype(jnp.int32)
    kept = jnp.sum(live_int)
    every = gather_directly(kept[None], "shard").reshape(shards)
    last = shards * rows - (jnp.sum(every) - jnp.cumsum(every))
    first = last - every
    rank = jnp.cumsum(live_int) - live_int
    place = jnp.where(live, (first[me] + rank) % rows, rows)
    pick = (local[:, None] == place[None, :]).astype(jnp.float32)
    block = jnp.dot(pick, values, precision=lax.Precision.HIGHEST)
    tiles = lax.all_to_all(block.reshape(shards, tile, width), "shard", 0, 0)
    sub = local % tile
    target = local // tile * rows + me * tile + sub
    fits = (first[local // tile][None, :] <= target[:, None]) & (target[:, None] < last[local // tile][None, :])
    mix = (fits & (sub[:, None] == sub[None, :])).astype(jnp.float32)
    mixed = jnp.dot(mix, tiles.reshape(rows, width), precision=lax.Precision.HIGHEST)
    packed = lax.all_to_all(mixed.reshape(shards, tile, width), "shard", 0, 0).reshape(rows, width)
    start = first[0]
    filled = jnp.clip((me + 1) * rows - start, 0, rows)
    row_live = (local >= rows - filled)[:, None]
    denom = jnp.maximum(filled.astype(jnp.float32), 1.0)
    mean = jnp.sum(packed, axis=0) / denom
    variance = jnp.sum(jnp.where(row_live, (packed - mean[None, :]) ** 2, 0.0), axis=0) / denom
    has_rows = filled > 0
    low = jnp.where(has_rows, jnp.min(jnp.where(row_live, packed, jnp.inf), axis=0), 0.0)
    high = jnp.where(has_rows, jnp.max(jnp.where(row_live, packed, -jnp.inf), axis=0), 0.0)
    span_stats = jnp.stack([mean, variance, low, high])[:, None, :]
    return (packed, span_stats)


def solution(mesh):
    in_specs = (P("shard", "col"), P(("shard", "col")), P("shard"))
    out_specs = (P("shard", "col"), P(None, "shard", "col"))
    return jax.shard_map(on_device, mesh=mesh, in_specs=in_specs, out_specs=out_specs, check_vma=False)
```

```python
import functools

import jax
import jax.numpy as jnp
from jax import lax
from jax.experimental import pallas as pl
from jax.experimental.pallas import tpu as pltpu
from jax.sharding import PartitionSpec as P

MESH = pl.DeviceIdType.MESH
CHUNKS = 2
SIZES = (8, 4, 2)


def hops(step):
    return sum(min(d, n - d) for d, n in zip(step[:2], SIZES[:2]))


STEPS = sorted(
    [(z, y, c) for z in range(8) for y in range(4) for c in range(2)][1:],
    key=lambda step: (-hops(step), step),
)


def iota(shape, dim):
    return lax.broadcasted_iota(jnp.int32, shape, dim)


def pieces(x):
    high = x.astype(jnp.bfloat16)
    rest = x - high.astype(jnp.float32)
    mid = rest.astype(jnp.bfloat16)
    low = (rest - mid.astype(jnp.float32)).astype(jnp.bfloat16)
    return jnp.concatenate([high, mid, low], axis=1)


def select(choice, parts):
    width = parts.shape[1] // 3
    out = jnp.dot(choice, parts, preferred_element_type=jnp.float32)
    return (out[:, :width] + out[:, width : 2 * width]) + out[:, 2 * width :]


def kernel(
    values_ref,
    mask_ref,
    counts_ref,
    packed_ref,
    stats_ref,
    values_buf,
    mask_own,
    mask_buf,
    counts_buf,
    kept_own,
    kept_buf,
    send_one,
    recv_one,
    send_two,
    recv_two,
    local_sem,
    mask_sem,
    kept_sem,
    one_sem,
    two_sem,
):
    rows, width = values_buf.shape
    shards = kept_buf.shape[0]
    unit = send_one.shape[2]
    span = shards * unit
    tile = rows // shards
    me = lax.axis_index("shard")
    col = lax.axis_index("col")

    load_mask = pltpu.make_async_copy(mask_ref, mask_own, local_sem.at[0])
    load_counts = pltpu.make_async_copy(counts_ref, counts_buf, local_sem.at[1])
    load_values = pltpu.make_async_copy(values_ref, values_buf, local_sem.at[2])
    load_mask.start()
    load_counts.start()
    load_values.start()

    z, y, c = me // 8, lax.rem(me // 2, 4), lax.rem(me, 2)
    peers = [
        lax.rem(z + dz, 8) * 8 + lax.rem(y + dy, 4) * 2 + lax.rem(c + dc, 2)
        for dz, dy, dc in STEPS
    ]
    cols = [lax.rem(col + d, 4) for d in (2, 1, 3)]

    barrier = pltpu.get_barrier_semaphore()
    for peer in peers:
        pl.semaphore_signal(barrier, inc=1, device_id={"shard": peer}, device_id_type=MESH)
    for peer in cols:
        pl.semaphore_signal(barrier, inc=1, device_id={"col": peer}, device_id_type=MESH)
    load_mask.wait()
    load_counts.wait()
    pl.semaphore_wait(barrier, len(peers) + len(cols))

    for peer in cols:
        pltpu.make_async_remote_copy(
            mask_own, mask_buf.at[col], mask_sem.at[0], mask_sem.at[1],
            device_id={"col": peer}, device_id_type=MESH,
        ).start()
    mask_buf[col] = mask_own[...]
    load_values.wait()
    parts = pieces(values_buf[...])
    three = mask_buf.at[pl.ds(0, len(cols))]
    pltpu.make_async_copy(three, three, mask_sem.at[1]).wait()

    groups = mask_buf.shape[0]
    mask = jnp.concatenate([mask_buf[g] for g in range(groups)], axis=0)
    row = iota((groups, width), 0) * width + iota((groups, width), 1)
    live = (mask == 1) & (row < counts_buf[0])
    live_part = jnp.where(live, 1.0, 0.0).astype(jnp.bfloat16)
    ahead = (iota((width, width), 0) < iota((width, width), 1)).astype(jnp.float32).astype(jnp.bfloat16)
    inside = jnp.dot(live_part, ahead, preferred_element_type=jnp.float32)
    ones = jnp.ones((width, width), jnp.bfloat16)
    whole = jnp.dot(live_part, ones, preferred_element_type=jnp.float32)
    kept = jnp.sum(whole, axis=0, keepdims=True)
    kept_own[...] = kept.astype(jnp.int32)
    for peer in peers:
        pltpu.make_async_remote_copy(
            kept_own, kept_buf.at[me], kept_sem.at[0], kept_sem.at[1],
            device_id={"shard": peer}, device_id_type=MESH,
        ).start()
    kept_buf[me] = kept_own[...]
    base = [jnp.zeros((1, width), jnp.float32)]
    for g in range(groups - 1):
        base.append(base[-1] + whole[g : g + 1])
    rank = (inside + jnp.concatenate(base, axis=0)).astype(jnp.int32)
    most = kept_buf.at[pl.ds(0, len(peers))]
    pltpu.make_async_copy(most, most, kept_sem.at[1]).wait()

    every = jnp.concatenate([kept_buf[i] for i in range(shards)], axis=0)
    shard = iota((shards, width), 0)
    mine = shards * rows - jnp.sum(jnp.where(shard >= me, every, 0), axis=0, keepdims=True)
    start = shards * rows - jnp.sum(every, axis=0, keepdims=True)
    target = mine + rank
    place = jnp.where(live, target - target // rows * rows, rows)

    index = iota((span, 1), 0)
    for h in range(CHUNKS):
        slot = index // unit * tile + unit * h + lax.rem(index, unit)
        choice = jnp.concatenate(
            [(slot == place[g : g + 1]).astype(jnp.float32).astype(jnp.bfloat16) for g in range(groups)], axis=1
        )
        send_one[h] = select(choice, parts).reshape(shards, unit, width)
        for peer in peers:
            pltpu.make_async_remote_copy(
                send_one.at[h, peer], recv_one.at[h, me], one_sem.at[0, h], one_sem.at[1, h],
                device_id={"shard": peer}, device_id_type=MESH,
            ).start()
        recv_one[h, me] = send_one[h, me]

    wide = jnp.concatenate([every] * max(1, span // width), axis=1)[:, :span]
    lane = iota((shards, span), 1) // unit
    source = iota((shards, span), 0)
    first = shards * rows - jnp.sum(jnp.where(source >= lane, wide, 0), axis=0, keepdims=True)
    last = shards * rows - jnp.sum(jnp.where(source > lane, wide, 0), axis=0, keepdims=True)
    inner = lax.rem(index, unit)
    same = inner == lax.rem(iota((1, span), 1), unit)
    for h in range(CHUNKS):
        part = recv_one.at[h, pl.ds(0, len(peers))]
        pltpu.make_async_copy(part, part, one_sem.at[1, h]).wait()
        goal = index // unit * rows + me * tile + unit * h + inner
        mix = (same & (first <= goal) & (goal < last)).astype(jnp.float32).astype(jnp.bfloat16)
        got = pieces(recv_one[h].reshape(span, width))
        send_two[h] = select(mix, got).reshape(shards, unit, width)
        for peer in peers:
            pltpu.make_async_remote_copy(
                send_two.at[h, peer], recv_two.at[h, me], two_sem.at[0, h], two_sem.at[1, h],
                device_id={"shard": peer}, device_id_type=MESH,
            ).start()
        recv_two[h, me] = send_two[h, me]
    for h in range(CHUNKS):
        part = recv_two.at[h, pl.ds(0, len(peers))]
        pltpu.make_async_copy(part, part, two_sem.at[1, h]).wait()
    packed = jnp.concatenate([recv_two[h] for h in range(CHUNKS)], axis=1).reshape(rows, width)
    packed_ref[...] = packed

    filled = jnp.clip((me + 1) * rows - start, 0, rows)
    row_live = iota((rows, width), 0) >= rows - filled
    scale = jnp.maximum(filled.astype(jnp.float32), 1.0)
    mean = jnp.sum(packed, axis=0, keepdims=True) / scale
    spread = jnp.where(row_live, (packed - mean) * (packed - mean), 0.0)
    variance = jnp.sum(spread, axis=0, keepdims=True) / scale
    low = jnp.min(jnp.where(row_live, packed, jnp.inf), axis=0, keepdims=True)
    high = jnp.max(jnp.where(row_live, packed, -jnp.inf), axis=0, keepdims=True)
    low = jnp.where(filled > 0, low, 0.0)
    high = jnp.where(filled > 0, high, 0.0)
    stats_ref[...] = jnp.concatenate([mean, variance, low, high], axis=0)

    for h in range(CHUNKS):
        part = recv_one.at[h, pl.ds(0, len(peers))]
        pltpu.make_async_copy(part, part, one_sem.at[0, h]).wait()
        pltpu.make_async_copy(part, part, two_sem.at[0, h]).wait()
    pltpu.make_async_copy(most, most, kept_sem.at[0]).wait()
    pltpu.make_async_copy(three, three, mask_sem.at[0]).wait()


def on_device(shards, groups, values, keep_mask, row_counts):
    rows, width = values.shape
    unit = rows // shards // CHUNKS
    blocks = pltpu.VMEM((CHUNKS, shards, unit, width), jnp.float32)
    packed, stats = pl.pallas_call(
        kernel,
        out_shape=(
            jax.ShapeDtypeStruct((rows, width), jnp.float32),
            jax.ShapeDtypeStruct((4, width), jnp.float32),
        ),
        in_specs=[pl.BlockSpec(memory_space=pl.ANY)] * 3,
        out_specs=(pl.BlockSpec(memory_space=pltpu.VMEM),) * 2,
        scratch_shapes=[
            pltpu.VMEM((rows, width), jnp.float32),
            pltpu.VMEM((1, width), jnp.int32),
            pltpu.VMEM((groups, 1, width), jnp.int32),
            pltpu.SMEM((1,), jnp.int32),
            pltpu.VMEM((1, width), jnp.int32),
            pltpu.VMEM((shards, 1, width), jnp.int32),
            blocks,
            blocks,
            blocks,
            blocks,
            pltpu.SemaphoreType.DMA((3,)),
            pltpu.SemaphoreType.DMA((2,)),
            pltpu.SemaphoreType.DMA((2,)),
            pltpu.SemaphoreType.DMA((2, CHUNKS)),
            pltpu.SemaphoreType.DMA((2, CHUNKS)),
        ],
        name="compact",
        compiler_params=pltpu.CompilerParams(collective_id=0, has_side_effects=True),
    )(values, keep_mask.reshape(1, width), row_counts)
    return packed, stats[:, None, :]


def solution(mesh):
    in_specs = (P("shard", "col"), P(("shard", "col")), P("shard"))
    out_specs = (P("shard", "col"), P(None, "shard", "col"))
    body = functools.partial(on_device, mesh.shape["shard"], mesh.shape["col"])
    return jax.shard_map(body, mesh=mesh, in_specs=in_specs, out_specs=out_specs, check_vma=False)
```

```python
import functools

import jax
import jax.numpy as jnp
from jax import lax
from jax.experimental import pallas as pl
from jax.experimental.pallas import tpu as pltpu
from jax.sharding import PartitionSpec as P

MESH = pl.DeviceIdType.MESH
CHUNKS = 4
SIZES = (8, 4, 2)


def hops(step):
    return sum(min(d, n - d) for d, n in zip(step[:2], SIZES[:2]))


STEPS = sorted(
    [(z, y, c) for z in range(8) for y in range(4) for c in range(2)][1:],
    key=lambda step: (-hops(step), step),
)


PLANE = sorted(
    [(y, c, x) for y in range(4) for c in range(2) for x in range(4)][1:],
    key=lambda step: (-min(step[0], 4 - step[0]) - min(step[2], 4 - step[2]), step),
)


def iota(shape, dim):
    return lax.broadcasted_iota(jnp.int32, shape, dim)


def pieces(x):
    high = x.astype(jnp.bfloat16)
    rest = x - high.astype(jnp.float32)
    mid = rest.astype(jnp.bfloat16)
    low = (rest - mid.astype(jnp.float32)).astype(jnp.bfloat16)
    return jnp.concatenate([high, mid, low], axis=1)


def select(choice, parts):
    width = parts.shape[1] // 3
    out = jnp.dot(choice, parts, preferred_element_type=jnp.float32)
    return (out[:, :width] + out[:, width : 2 * width]) + out[:, 2 * width :]


def kernel(
    values_ref,
    mask_ref,
    counts_ref,
    packed_ref,
    stats_ref,
    values_buf,
    mask_own,
    mask_buf,
    counts_buf,
    kept_own,
    line_buf,
    line_own,
    plane_buf,
    send_one,
    recv_one,
    send_two,
    recv_two,
    local_sem,
    mask_sem,
    line_sem,
    plane_sem,
    one_sem,
    two_sem,
):
    rows, width = values_buf.shape
    shards = send_one.shape[1]
    groups = mask_buf.shape[0]
    depth, breadth = SIZES[0], SIZES[1] * SIZES[2]
    unit = send_one.shape[2]
    span = shards * unit
    tile = rows // shards
    me = lax.axis_index("shard")
    col = lax.axis_index("col")

    load_mask = pltpu.make_async_copy(mask_ref, mask_own, local_sem.at[0])
    load_counts = pltpu.make_async_copy(counts_ref, counts_buf, local_sem.at[1])
    load_values = pltpu.make_async_copy(values_ref, values_buf, local_sem.at[2])
    load_mask.start()
    load_counts.start()
    load_values.start()

    z, y, c = me // 8, lax.rem(me // 2, 4), lax.rem(me, 2)
    peers = [
        lax.rem(z + dz, 8) * 8 + lax.rem(y + dy, 4) * 2 + lax.rem(c + dc, 2)
        for dz, dy, dc in STEPS
    ]
    cols = [lax.rem(col + d, 4) for d in (2, 1, 3)]
    lines = [lax.rem(z + dz, 8) * 8 + lax.rem(me, 8) for dz in (4, 3, 5, 2, 6, 1, 7)]
    planes = [
        {"shard": z * 8 + lax.rem(y + dy, 4) * 2 + lax.rem(c + dc, 2), "col": lax.rem(col + dx, 4)}
        for dy, dc, dx in PLANE
    ]

    barrier = pltpu.get_barrier_semaphore()
    for peer in lines:
        pl.semaphore_signal(barrier, inc=1, device_id={"shard": peer}, device_id_type=MESH)
    for peer in planes:
        pl.semaphore_signal(barrier, inc=1, device_id=peer, device_id_type=MESH)
    load_mask.wait()
    load_counts.wait()
    present = counts_buf[0]
    mine = (mask_own[...] == 1) & (col * width + iota((1, width), 1) < present)
    kept = jnp.sum(jnp.where(mine, 1, 0), axis=1, keepdims=True)
    kept_own[...] = jnp.broadcast_to(kept, (1, width))
    pl.semaphore_wait(barrier, len(lines) + len(planes))

    for peer in lines:
        pltpu.make_async_remote_copy(
            kept_own, line_buf.at[z], line_sem.at[0], line_sem.at[1],
            device_id={"shard": peer}, device_id_type=MESH,
        ).start()
    for peer in cols:
        pltpu.make_async_remote_copy(
            mask_own, mask_buf.at[col], mask_sem.at[0], mask_sem.at[1],
            device_id={"col": peer}, device_id_type=MESH,
        ).start()
    line_buf[z] = kept_own[...]
    mask_buf[col] = mask_own[...]
    line_part = line_buf.at[pl.ds(0, len(lines))]
    pltpu.make_async_copy(line_part, line_part, line_sem.at[1]).wait()
    level = iota((1, width), 1) // (width // depth)
    line = line_buf[0]
    for k in range(1, depth):
        line = jnp.where(level == k, line_buf[k], line)
    line_own[...] = line
    place_in_plane = lax.rem(me, breadth) * groups + col
    for peer in planes:
        pltpu.make_async_remote_copy(
            line_own, plane_buf.at[place_in_plane], plane_sem.at[0], plane_sem.at[1],
            device_id=peer, device_id_type=MESH,
        ).start()
    plane_buf[place_in_plane] = line_own[...]

    load_values.wait()
    parts = pieces(values_buf[...])
    three = mask_buf.at[pl.ds(0, len(cols))]
    pltpu.make_async_copy(three, three, mask_sem.at[1]).wait()
    mask = jnp.concatenate([mask_buf[g] for g in range(groups)], axis=0)
    row = iota((groups, width), 0) * width + iota((groups, width), 1)
    live = (mask == 1) & (row < present)
    live_part = jnp.where(live, 1.0, 0.0).astype(jnp.bfloat16)
    ahead = (iota((width, width), 0) < iota((width, width), 1)).astype(jnp.float32).astype(jnp.bfloat16)
    inside = jnp.dot(live_part, ahead, preferred_element_type=jnp.float32)
    ones = jnp.ones((width, width), jnp.bfloat16)
    whole = jnp.dot(live_part, ones, preferred_element_type=jnp.float32)
    base = [jnp.zeros((1, width), jnp.float32)]
    for g in range(groups - 1):
        base.append(base[-1] + whole[g : g + 1])
    rank = (inside + jnp.concatenate(base, axis=0)).astype(jnp.int32)
    plane_part = plane_buf.at[pl.ds(0, len(planes))]
    pltpu.make_async_copy(plane_part, plane_part, plane_sem.at[1]).wait()

    plane = [
        sum(plane_buf[b * groups + g] for g in range(1, groups)) + plane_buf[b * groups] for b in range(breadth)
    ]
    plane = jnp.concatenate(plane, axis=0)
    every = jnp.concatenate(
        [
            jnp.broadcast_to(plane[:, k * (width // depth) : k * (width // depth) + 1], (breadth, width))
            for k in range(depth)
        ],
        axis=0,
    )
    shard = iota((shards, width), 0)
    mine = shards * rows - jnp.sum(jnp.where(shard >= me, every, 0), axis=0, keepdims=True)
    start = shards * rows - jnp.sum(every, axis=0, keepdims=True)
    target = mine + rank
    place = jnp.where(live, target - target // rows * rows, rows)

    index = iota((span, 1), 0)
    for h in range(CHUNKS):
        slot = index // unit * tile + unit * h + lax.rem(index, unit)
        choice = jnp.concatenate(
            [(slot == place[g : g + 1]).astype(jnp.float32).astype(jnp.bfloat16) for g in range(groups)], axis=1
        )
        send_one[h] = select(choice, parts).reshape(shards, unit, width)
        for peer in peers:
            pltpu.make_async_remote_copy(
                send_one.at[h, peer], recv_one.at[h, me], one_sem.at[0, h], one_sem.at[1, h],
                device_id={"shard": peer}, device_id_type=MESH,
            ).start()
        recv_one[h, me] = send_one[h, me]

    wide = jnp.concatenate([every] * max(1, span // width), axis=1)[:, :span]
    lane = iota((shards, span), 1) // unit
    source = iota((shards, span), 0)
    first = shards * rows - jnp.sum(jnp.where(source >= lane, wide, 0), axis=0, keepdims=True)
    last = shards * rows - jnp.sum(jnp.where(source > lane, wide, 0), axis=0, keepdims=True)
    inner = lax.rem(index, unit)
    same = inner == lax.rem(iota((1, span), 1), unit)
    for h in range(CHUNKS):
        part = recv_one.at[h, pl.ds(0, len(peers))]
        pltpu.make_async_copy(part, part, one_sem.at[1, h]).wait()
        goal = index // unit * rows + me * tile + unit * h + inner
        mix = (same & (first <= goal) & (goal < last)).astype(jnp.float32).astype(jnp.bfloat16)
        got = pieces(recv_one[h].reshape(span, width))
        send_two[h] = select(mix, got).reshape(shards, unit, width)
        for peer in peers:
            pltpu.make_async_remote_copy(
                send_two.at[h, peer], recv_two.at[h, me], two_sem.at[0, h], two_sem.at[1, h],
                device_id={"shard": peer}, device_id_type=MESH,
            ).start()
        recv_two[h, me] = send_two[h, me]
    for h in range(CHUNKS):
        part = recv_two.at[h, pl.ds(0, len(peers))]
        pltpu.make_async_copy(part, part, two_sem.at[1, h]).wait()
    packed = jnp.concatenate([recv_two[h] for h in range(CHUNKS)], axis=1).reshape(rows, width)
    packed_ref[...] = packed

    filled = jnp.clip((me + 1) * rows - start, 0, rows)
    row_live = iota((rows, width), 0) >= rows - filled
    scale = jnp.maximum(filled.astype(jnp.float32), 1.0)
    mean = jnp.sum(packed, axis=0, keepdims=True) / scale
    spread = jnp.where(row_live, (packed - mean) * (packed - mean), 0.0)
    variance = jnp.sum(spread, axis=0, keepdims=True) / scale
    low = jnp.min(jnp.where(row_live, packed, jnp.inf), axis=0, keepdims=True)
    high = jnp.max(jnp.where(row_live, packed, -jnp.inf), axis=0, keepdims=True)
    low = jnp.where(filled > 0, low, 0.0)
    high = jnp.where(filled > 0, high, 0.0)
    for place, stat in enumerate((mean, variance, low, high)):
        stats_ref[place] = stat

    for h in range(CHUNKS):
        part = recv_one.at[h, pl.ds(0, len(peers))]
        pltpu.make_async_copy(part, part, one_sem.at[0, h]).wait()
        pltpu.make_async_copy(part, part, two_sem.at[0, h]).wait()
    pltpu.make_async_copy(line_part, line_part, line_sem.at[0]).wait()
    pltpu.make_async_copy(plane_part, plane_part, plane_sem.at[0]).wait()
    pltpu.make_async_copy(three, three, mask_sem.at[0]).wait()


def deliver(packed_ref, stats_ref, packed_out, stats_out, sem):
    rows = pltpu.make_async_copy(packed_ref, packed_out, sem.at[0])
    stats = pltpu.make_async_copy(stats_ref, stats_out, sem.at[1])
    rows.start()
    stats.start()
    rows.wait()
    stats.wait()


def on_device(shards, groups, values, keep_mask, row_counts):
    rows, width = values.shape
    unit = rows // shards // CHUNKS
    blocks = pltpu.VMEM((CHUNKS, shards, unit, width), jnp.float32)
    packed, stats = pl.pallas_call(
        kernel,
        out_shape=(
            jax.ShapeDtypeStruct((rows, width), jnp.float32),
            jax.ShapeDtypeStruct((4, 1, width), jnp.float32),
        ),
        in_specs=[pl.BlockSpec(memory_space=pltpu.HBM)] * 3,
        out_specs=(pl.BlockSpec(memory_space=pltpu.VMEM),) * 2,
        scratch_shapes=[
            pltpu.VMEM((rows, width), jnp.float32),
            pltpu.VMEM((1, width), jnp.int32),
            pltpu.VMEM((groups, 1, width), jnp.int32),
            pltpu.SMEM((1,), jnp.int32),
            pltpu.VMEM((1, width), jnp.int32),
            pltpu.VMEM((SIZES[0], 1, width), jnp.int32),
            pltpu.VMEM((1, width), jnp.int32),
            pltpu.VMEM((SIZES[1] * SIZES[2] * groups, 1, width), jnp.int32),
            blocks,
            blocks,
            blocks,
            blocks,
            pltpu.SemaphoreType.DMA((3,)),
            pltpu.SemaphoreType.DMA((2,)),
            pltpu.SemaphoreType.DMA((2,)),
            pltpu.SemaphoreType.DMA((2,)),
            pltpu.SemaphoreType.DMA((2, CHUNKS)),
            pltpu.SemaphoreType.DMA((2, CHUNKS)),
        ],
        name="compact",
        compiler_params=pltpu.CompilerParams(collective_id=0, has_side_effects=True, vmem_limit_bytes=8 * 1024 * 1024),
    )(
        pltpu.with_memory_space_constraint(values, pltpu.HBM),
        pltpu.with_memory_space_constraint(keep_mask.reshape(1, width), pltpu.HBM),
        row_counts,
    )
    whole = pl.BlockSpec(memory_space=pltpu.VMEM)
    return pl.pallas_call(
        deliver,
        out_shape=(
            jax.ShapeDtypeStruct((rows, width), jnp.float32),
            jax.ShapeDtypeStruct((4, 1, width), jnp.float32),
        ),
        in_specs=[pl.BlockSpec(memory_space=pl.ANY)] * 2,
        out_specs=(pl.BlockSpec(memory_space=pltpu.HBM),) * 2,
        scratch_shapes=[pltpu.SemaphoreType.DMA((2,))],
        name="deliver",
        compiler_params=pltpu.CompilerParams(vmem_limit_bytes=1024 * 1024),
    )(packed, stats)


def solution(mesh):
    in_specs = (P("shard", "col"), P(("shard", "col")), P("shard"))
    out_specs = (P("shard", "col"), P(None, "shard", "col"))
    body = functools.partial(on_device, mesh.shape["shard"], mesh.shape["col"])
    return jax.shard_map(body, mesh=mesh, in_specs=in_specs, out_specs=out_specs, check_vma=False)
```

```python
import functools

import jax
import jax.numpy as jnp
from jax import lax
from jax.experimental import pallas as pl
from jax.experimental.pallas import tpu as pltpu
from jax.sharding import PartitionSpec as P

MESH = pl.DeviceIdType.MESH
CHUNKS = 4
SIZES = (8, 4, 2)


def hops(step):
    return sum(min(d, n - d) for d, n in zip(step[:2], SIZES[:2]))


STEPS = sorted(
    [(z, y, c) for z in range(8) for y in range(4) for c in range(2)][1:],
    key=lambda step: (-hops(step), -min(step[0], 8 - step[0]), step),
)


PLANE = sorted(
    [(y, c, x) for y in range(4) for c in range(2) for x in range(4)][1:],
    key=lambda step: (-min(step[0], 4 - step[0]) - min(step[2], 4 - step[2]), step),
)


def iota(shape, dim):
    return lax.broadcasted_iota(jnp.int32, shape, dim)


def pieces(x):
    high = x.astype(jnp.bfloat16)
    rest = x - high.astype(jnp.float32)
    mid = rest.astype(jnp.bfloat16)
    low = (rest - mid.astype(jnp.float32)).astype(jnp.bfloat16)
    return jnp.concatenate([high, mid, low], axis=1)


def select(choice, parts):
    width = parts.shape[1] // 3
    out = jnp.dot(choice, parts, preferred_element_type=jnp.float32)
    return (out[:, :width] + out[:, width : 2 * width]) + out[:, 2 * width :]


def kernel(
    values_ref,
    mask_ref,
    counts_ref,
    packed_ref,
    filled_ref,
    values_buf,
    mask_own,
    mask_buf,
    counts_buf,
    kept_own,
    line_buf,
    line_own,
    plane_buf,
    send_one,
    recv_one,
    send_two,
    local_sem,
    mask_sem,
    line_sem,
    plane_sem,
    one_sem,
    two_sem,
):
    rows, width = values_buf.shape
    shards = send_one.shape[1]
    groups = mask_buf.shape[0]
    depth, breadth = SIZES[0], SIZES[1] * SIZES[2]
    unit = send_one.shape[2]
    span = shards * unit
    tile = rows // shards
    me = lax.axis_index("shard")
    col = lax.axis_index("col")

    load_mask = pltpu.make_async_copy(mask_ref, mask_own, local_sem.at[0])
    load_counts = pltpu.make_async_copy(counts_ref, counts_buf, local_sem.at[1])
    load_values = pltpu.make_async_copy(values_ref, values_buf, local_sem.at[2])
    load_mask.start()
    load_counts.start()
    load_values.start()

    z, y, c = me // 8, lax.rem(me // 2, 4), lax.rem(me, 2)
    peers = [
        lax.rem(z + dz, 8) * 8 + lax.rem(y + dy, 4) * 2 + lax.rem(c + dc, 2)
        for dz, dy, dc in STEPS
    ]
    cols = [lax.rem(col + d, 4) for d in (2, 1, 3)]
    lines = [lax.rem(z + dz, 8) * 8 + lax.rem(me, 8) for dz in (4, 3, 5, 2, 6, 1, 7)]
    planes = [
        {"shard": z * 8 + lax.rem(y + dy, 4) * 2 + lax.rem(c + dc, 2), "col": lax.rem(col + dx, 4)}
        for dy, dc, dx in PLANE
    ]

    barrier = pltpu.get_barrier_semaphore()
    for peer in lines:
        pl.semaphore_signal(barrier, inc=1, device_id={"shard": peer}, device_id_type=MESH)
    for peer in planes:
        pl.semaphore_signal(barrier, inc=1, device_id=peer, device_id_type=MESH)
    load_mask.wait()
    load_counts.wait()
    present = counts_buf[0]
    mine = (mask_own[...] == 1) & (col * width + iota((1, width), 1) < present)
    kept = jnp.sum(jnp.where(mine, 1, 0), axis=1, keepdims=True)
    kept_own[...] = jnp.broadcast_to(kept, (1, width))
    pl.semaphore_wait(barrier, len(lines) + len(planes))

    for peer in lines:
        pltpu.make_async_remote_copy(
            kept_own, line_buf.at[z], line_sem.at[0], line_sem.at[1],
            device_id={"shard": peer}, device_id_type=MESH,
        ).start()
    for peer in cols:
        pltpu.make_async_remote_copy(
            mask_own, mask_buf.at[col], mask_sem.at[0], mask_sem.at[1],
            device_id={"col": peer}, device_id_type=MESH,
        ).start()
    line_buf[z] = kept_own[...]
    mask_buf[col] = mask_own[...]
    line_part = line_buf.at[pl.ds(0, len(lines))]
    pltpu.make_async_copy(line_part, line_part, line_sem.at[1]).wait()
    level = iota((1, width), 1) // (width // depth)
    line = line_buf[0]
    for k in range(1, depth):
        line = jnp.where(level == k, line_buf[k], line)
    line_own[...] = line
    place_in_plane = lax.rem(me, breadth) * groups + col
    for peer in planes:
        pltpu.make_async_remote_copy(
            line_own, plane_buf.at[place_in_plane], plane_sem.at[0], plane_sem.at[1],
            device_id=peer, device_id_type=MESH,
        ).start()
    plane_buf[place_in_plane] = line_own[...]

    load_values.wait()
    parts = pieces(values_buf[...])
    three = mask_buf.at[pl.ds(0, len(cols))]
    pltpu.make_async_copy(three, three, mask_sem.at[1]).wait()
    mask = jnp.concatenate([mask_buf[g] for g in range(groups)], axis=0)
    row = iota((groups, width), 0) * width + iota((groups, width), 1)
    live = (mask == 1) & (row < present)
    live_part = jnp.where(live, 1.0, 0.0).astype(jnp.bfloat16)
    ahead = (iota((width, width), 0) < iota((width, width), 1)).astype(jnp.float32).astype(jnp.bfloat16)
    inside = jnp.dot(live_part, ahead, preferred_element_type=jnp.float32)
    ones = jnp.ones((width, width), jnp.bfloat16)
    whole = jnp.dot(live_part, ones, preferred_element_type=jnp.float32)
    base = [jnp.zeros((1, width), jnp.float32)]
    for g in range(groups - 1):
        base.append(base[-1] + whole[g : g + 1])
    rank = (inside + jnp.concatenate(base, axis=0)).astype(jnp.int32)
    plane_part = plane_buf.at[pl.ds(0, len(planes))]
    pltpu.make_async_copy(plane_part, plane_part, plane_sem.at[1]).wait()

    plane = [
        sum(plane_buf[b * groups + g] for g in range(1, groups)) + plane_buf[b * groups] for b in range(breadth)
    ]
    plane = jnp.concatenate(plane, axis=0)
    every = jnp.concatenate(
        [
            jnp.broadcast_to(plane[:, k * (width // depth) : k * (width // depth) + 1], (breadth, width))
            for k in range(depth)
        ],
        axis=0,
    )
    shard = iota((shards, width), 0)
    mine = shards * rows - jnp.sum(jnp.where(shard >= me, every, 0), axis=0, keepdims=True)
    start = shards * rows - jnp.sum(every, axis=0, keepdims=True)
    target = mine + rank
    place = jnp.where(live, target - target // rows * rows, rows)

    index = iota((span, 1), 0)
    for h in range(CHUNKS):
        slot = index // unit * tile + unit * h + lax.rem(index, unit)
        choice = jnp.concatenate(
            [(slot == place[g : g + 1]).astype(jnp.float32).astype(jnp.bfloat16) for g in range(groups)], axis=1
        )
        send_one[h] = select(choice, parts).reshape(shards, unit, width)
        for peer in peers:
            pltpu.make_async_remote_copy(
                send_one.at[h, peer], recv_one.at[h, me], one_sem.at[0, h], one_sem.at[1, h],
                device_id={"shard": peer}, device_id_type=MESH,
            ).start()
        recv_one[h, me] = send_one[h, me]

    wide = jnp.concatenate([every] * max(1, span // width), axis=1)[:, :span]
    lane = iota((shards, span), 1) // unit
    source = iota((shards, span), 0)
    first = shards * rows - jnp.sum(jnp.where(source >= lane, wide, 0), axis=0, keepdims=True)
    last = shards * rows - jnp.sum(jnp.where(source > lane, wide, 0), axis=0, keepdims=True)
    inner = lax.rem(index, unit)
    same = inner == lax.rem(iota((1, span), 1), unit)
    for h in range(CHUNKS):
        part = recv_one.at[h, pl.ds(0, len(peers))]
        pltpu.make_async_copy(part, part, one_sem.at[1, h]).wait()
        goal = index // unit * rows + me * tile + unit * h + inner
        mix = (same & (first <= goal) & (goal < last)).astype(jnp.float32).astype(jnp.bfloat16)
        got = pieces(recv_one[h].reshape(span, width))
        send_two[h] = select(mix, got).reshape(shards, unit, width)
        for peer in peers:
            pltpu.make_async_remote_copy(
                send_two.at[h, peer], packed_ref.at[me, pl.ds(unit * h, unit)], two_sem.at[0, h], two_sem.at[1, h],
                device_id={"shard": peer}, device_id_type=MESH,
            ).start()
        packed_ref[me, unit * h : unit * (h + 1)] = send_two[h, me]
    filled_ref[...] = jnp.clip((me + 1) * rows - start, 0, rows)
    for h in range(CHUNKS):
        part = packed_ref.at[pl.ds(0, len(peers)), pl.ds(unit * h, unit)]
        pltpu.make_async_copy(part, part, two_sem.at[1, h]).wait()
    for h in range(CHUNKS):
        part = recv_one.at[h, pl.ds(0, len(peers))]
        pltpu.make_async_copy(part, part, one_sem.at[0, h]).wait()
        pltpu.make_async_copy(part, part, two_sem.at[0, h]).wait()
    pltpu.make_async_copy(line_part, line_part, line_sem.at[0]).wait()
    pltpu.make_async_copy(plane_part, plane_part, plane_sem.at[0]).wait()
    pltpu.make_async_copy(three, three, mask_sem.at[0]).wait()


def deliver(packed_ref, filled_ref, packed_out, stats_out, stats_buf, sem):
    shards, tile, width = packed_ref.shape
    rows = shards * tile
    leave = pltpu.make_async_copy(packed_ref, packed_out, sem.at[0])
    leave.start()
    filled = filled_ref[...]
    scale = jnp.maximum(filled.astype(jnp.float32), 1.0)
    slot = iota((shards, tile, width), 0) * tile + iota((shards, tile, width), 1)
    row_live = slot >= (rows - filled)[:, None]
    packed = packed_ref[...]
    total = jnp.sum(jnp.sum(packed, axis=0), axis=0, keepdims=True)
    low = jnp.min(jnp.min(jnp.where(row_live, packed, jnp.inf), axis=0), axis=0, keepdims=True)
    high = jnp.max(jnp.max(jnp.where(row_live, packed, -jnp.inf), axis=0), axis=0, keepdims=True)
    mean = total / scale
    away = packed - mean[None]
    spread = jnp.where(row_live, away * away, 0.0)
    variance = jnp.sum(jnp.sum(spread, axis=0), axis=0, keepdims=True) / scale
    low = jnp.where(filled > 0, low, 0.0)
    high = jnp.where(filled > 0, high, 0.0)
    for place, stat in enumerate((mean, variance, low, high)):
        stats_buf[place] = stat
    stats = pltpu.make_async_copy(stats_buf, stats_out, sem.at[1])
    stats.start()
    leave.wait()
    stats.wait()


def on_device(shards, groups, values, keep_mask, row_counts):
    rows, width = values.shape
    unit = rows // shards // CHUNKS
    blocks = pltpu.VMEM((CHUNKS, shards, unit, width), jnp.float32)
    packed, filled = pl.pallas_call(
        kernel,
        out_shape=(
            jax.ShapeDtypeStruct((shards, rows // shards, width), jnp.float32),
            jax.ShapeDtypeStruct((1, width), jnp.int32),
        ),
        in_specs=[pl.BlockSpec(memory_space=pltpu.HBM)] * 3,
        out_specs=(pl.BlockSpec(memory_space=pltpu.VMEM),) * 2,
        scratch_shapes=[
            pltpu.VMEM((rows, width), jnp.float32),
            pltpu.VMEM((1, width), jnp.int32),
            pltpu.VMEM((groups, 1, width), jnp.int32),
            pltpu.SMEM((1,), jnp.int32),
            pltpu.VMEM((1, width), jnp.int32),
            pltpu.VMEM((SIZES[0], 1, width), jnp.int32),
            pltpu.VMEM((1, width), jnp.int32),
            pltpu.VMEM((SIZES[1] * SIZES[2] * groups, 1, width), jnp.int32),
            blocks,
            blocks,
            blocks,
            pltpu.SemaphoreType.DMA((3,)),
            pltpu.SemaphoreType.DMA((2,)),
            pltpu.SemaphoreType.DMA((2,)),
            pltpu.SemaphoreType.DMA((2,)),
            pltpu.SemaphoreType.DMA((2, CHUNKS)),
            pltpu.SemaphoreType.DMA((2, CHUNKS)),
        ],
        name="compact",
        compiler_params=pltpu.CompilerParams(collective_id=0, has_side_effects=True, vmem_limit_bytes=8 * 1024 * 1024),
    )(
        pltpu.with_memory_space_constraint(values, pltpu.HBM),
        pltpu.with_memory_space_constraint(keep_mask.reshape(1, width), pltpu.HBM),
        row_counts,
    )
    packed, stats = pl.pallas_call(
        deliver,
        out_shape=(
            jax.ShapeDtypeStruct((shards, rows // shards, width), jnp.float32),
            jax.ShapeDtypeStruct((4, 1, width), jnp.float32),
        ),
        in_specs=[pl.BlockSpec(memory_space=pltpu.VMEM)] * 2,
        out_specs=(pl.BlockSpec(memory_space=pltpu.HBM),) * 2,
        scratch_shapes=[pltpu.VMEM((4, 1, width), jnp.float32), pltpu.SemaphoreType.DMA((2,))],
        name="deliver",
        compiler_params=pltpu.CompilerParams(vmem_limit_bytes=1024 * 1024),
    )(packed, filled)
    return packed.reshape(rows, width), stats


def solution(mesh):
    in_specs = (P("shard", "col"), P(("shard", "col")), P("shard"))
    out_specs = (P("shard", "col"), P(None, "shard", "col"))
    body = functools.partial(on_device, mesh.shape["shard"], mesh.shape["col"])
    return jax.shard_map(body, mesh=mesh, in_specs=in_specs, out_specs=out_specs, check_vma=False)
```

```python
import functools

import jax
import jax.numpy as jnp
from jax import lax
from jax.experimental import pallas as pl
from jax.experimental.pallas import tpu as pltpu
from jax.sharding import PartitionSpec as P

MESH = pl.DeviceIdType.MESH
CHUNKS = 4
SIZES = (8, 4, 2)


def hops(step):
    return sum(min(d, n - d) for d, n in zip(step[:2], SIZES[:2]))


STEPS = sorted(
    [(z, y, c) for z in range(8) for y in range(4) for c in range(2)][1:],
    key=lambda step: (-hops(step), (step[0] * 5 + step[1] * 3 + step[2] * 7) % 11, step),
)


PLANE = sorted(
    [(y, c, x) for y in range(4) for c in range(2) for x in range(4)][1:],
    key=lambda step: (-min(step[0], 4 - step[0]) - min(step[2], 4 - step[2]), step),
)


def iota(shape, dim):
    return lax.broadcasted_iota(jnp.int32, shape, dim)


def pieces(x):
    high = x.astype(jnp.bfloat16)
    rest = x - high.astype(jnp.float32)
    mid = rest.astype(jnp.bfloat16)
    low = (rest - mid.astype(jnp.float32)).astype(jnp.bfloat16)
    return jnp.concatenate([high, mid, low], axis=1)


def select(choice, parts):
    width = parts.shape[1] // 3
    out = jnp.dot(choice, parts, preferred_element_type=jnp.float32)
    return (out[:, :width] + out[:, width : 2 * width]) + out[:, 2 * width :]


def kernel(
    values_ref,
    mask_ref,
    counts_ref,
    packed_ref,
    filled_ref,
    values_buf,
    mask_own,
    mask_buf,
    counts_buf,
    kept_own,
    line_buf,
    line_own,
    plane_buf,
    send_one,
    recv_one,
    send_two,
    local_sem,
    mask_sem,
    line_sem,
    plane_sem,
    one_sem,
    two_sem,
):
    rows, width = values_buf.shape
    shards = send_one.shape[1]
    groups = mask_buf.shape[0]
    depth, breadth = SIZES[0], SIZES[1] * SIZES[2]
    unit = send_one.shape[2]
    span = shards * unit
    tile = rows // shards
    me = lax.axis_index("shard")
    col = lax.axis_index("col")

    load_mask = pltpu.make_async_copy(mask_ref, mask_own, local_sem.at[0])
    load_counts = pltpu.make_async_copy(counts_ref, counts_buf, local_sem.at[1])
    load_values = pltpu.make_async_copy(values_ref, values_buf, local_sem.at[2])
    load_mask.start()
    load_counts.start()
    load_values.start()

    z, y, c = me // 8, lax.rem(me // 2, 4), lax.rem(me, 2)
    peers = [
        lax.rem(z + dz, 8) * 8 + lax.rem(y + dy, 4) * 2 + lax.rem(c + dc, 2)
        for dz, dy, dc in STEPS
    ]
    cols = [lax.rem(col + d, 4) for d in (2, 1, 3)]
    lines = [lax.rem(z + dz, 8) * 8 + lax.rem(me, 8) for dz in (4, 3, 5, 2, 6, 1, 7)]
    planes = [
        {"shard": z * 8 + lax.rem(y + dy, 4) * 2 + lax.rem(c + dc, 2), "col": lax.rem(col + dx, 4)}
        for dy, dc, dx in PLANE
    ]

    near = [z * 8 + lax.rem(y + dy, 4) * 2 + lax.rem(c + dc, 2) for dy, dc in ((2, 1), (2, 0), (1, 1), (3, 1), (1, 0), (3, 0), (0, 1))]
    climb = [
        (step - 1 + (step + 7 - z) // 8) * 8 + lax.rem(y + dy, 4) * 2 + lax.rem(c + dc, 2)
        for step in range(1, 8)
        for dy in (2, 1, 3, 0)
        for dc in (1, 0)
    ]
    early, late = near + climb[: 32], climb[32 :]

    barrier = pltpu.get_barrier_semaphore()
    for peer in lines:
        pl.semaphore_signal(barrier, inc=1, device_id={"shard": peer}, device_id_type=MESH)
    for peer in planes:
        pl.semaphore_signal(barrier, inc=1, device_id=peer, device_id_type=MESH)
    load_mask.wait()
    load_counts.wait()
    present = counts_buf[0]
    mine = (mask_own[...] == 1) & (col * width + iota((1, width), 1) < present)
    kept = jnp.sum(jnp.where(mine, 1, 0), axis=1, keepdims=True)
    kept_own[...] = jnp.broadcast_to(kept, (1, width))
    pl.semaphore_wait(barrier, len(lines) + len(planes))

    for peer in lines:
        pltpu.make_async_remote_copy(
            kept_own, line_buf.at[z], line_sem.at[0], line_sem.at[1],
            device_id={"shard": peer}, device_id_type=MESH,
        ).start()
    for peer in cols:
        pltpu.make_async_remote_copy(
            mask_own, mask_buf.at[col], mask_sem.at[0], mask_sem.at[1],
            device_id={"col": peer}, device_id_type=MESH,
        ).start()
    line_buf[z] = kept_own[...]
    mask_buf[col] = mask_own[...]
    line_part = line_buf.at[pl.ds(0, len(lines))]
    pltpu.make_async_copy(line_part, line_part, line_sem.at[1]).wait()
    level = iota((1, width), 1) // (width // depth)
    line = line_buf[0]
    for k in range(1, depth):
        line = jnp.where(level == k, line_buf[k], line)
    line_own[...] = line
    place_in_plane = lax.rem(me, breadth) * groups + col
    for peer in planes:
        pltpu.make_async_remote_copy(
            line_own, plane_buf.at[place_in_plane], plane_sem.at[0], plane_sem.at[1],
            device_id=peer, device_id_type=MESH,
        ).start()
    plane_buf[place_in_plane] = line_own[...]

    load_values.wait()
    parts = pieces(values_buf[...])
    three = mask_buf.at[pl.ds(0, len(cols))]
    pltpu.make_async_copy(three, three, mask_sem.at[1]).wait()
    mask = jnp.concatenate([mask_buf[g] for g in range(groups)], axis=0)
    row = iota((groups, width), 0) * width + iota((groups, width), 1)
    live = (mask == 1) & (row < present)
    live_part = jnp.where(live, 1.0, 0.0).astype(jnp.bfloat16)
    ahead = (iota((width, width), 0) < iota((width, width), 1)).astype(jnp.float32).astype(jnp.bfloat16)
    inside = jnp.dot(live_part, ahead, preferred_element_type=jnp.float32)
    ones = jnp.ones((width, width), jnp.bfloat16)
    whole = jnp.dot(live_part, ones, preferred_element_type=jnp.float32)
    base = [jnp.zeros((1, width), jnp.float32)]
    for g in range(groups - 1):
        base.append(base[-1] + whole[g : g + 1])
    rank = (inside + jnp.concatenate(base, axis=0)).astype(jnp.int32)
    plane_part = plane_buf.at[pl.ds(0, len(planes))]
    pltpu.make_async_copy(plane_part, plane_part, plane_sem.at[1]).wait()

    plane = [
        sum(plane_buf[b * groups + g] for g in range(1, groups)) + plane_buf[b * groups] for b in range(breadth)
    ]
    plane = jnp.concatenate(plane, axis=0)
    every = jnp.concatenate(
        [
            jnp.broadcast_to(plane[:, k * (width // depth) : k * (width // depth) + 1], (breadth, width))
            for k in range(depth)
        ],
        axis=0,
    )
    shard = iota((shards, width), 0)
    mine = shards * rows - jnp.sum(jnp.where(shard >= me, every, 0), axis=0, keepdims=True)
    start = shards * rows - jnp.sum(every, axis=0, keepdims=True)
    target = mine + rank
    place = jnp.where(live, target - target // rows * rows, rows)

    index = iota((span, 1), 0)
    for h in range(CHUNKS):
        slot = index // unit * tile + unit * h + lax.rem(index, unit)
        choice = jnp.concatenate(
            [(slot == place[g : g + 1]).astype(jnp.float32).astype(jnp.bfloat16) for g in range(groups)], axis=1
        )
        send_one[h] = select(choice, parts).reshape(shards, unit, width)
        for peer in peers:
            pltpu.make_async_remote_copy(
                send_one.at[h, peer], recv_one.at[h, me], one_sem.at[0, h], one_sem.at[1, h],
                device_id={"shard": peer}, device_id_type=MESH,
            ).start()
        recv_one[h, me] = send_one[h, me]

    wide = jnp.concatenate([every] * max(1, span // width), axis=1)[:, :span]
    lane = iota((shards, span), 1) // unit
    source = iota((shards, span), 0)
    first = shards * rows - jnp.sum(jnp.where(source >= lane, wide, 0), axis=0, keepdims=True)
    last = shards * rows - jnp.sum(jnp.where(source > lane, wide, 0), axis=0, keepdims=True)
    inner = lax.rem(index, unit)
    same = inner == lax.rem(iota((1, span), 1), unit)
    for h in range(CHUNKS):
        part = recv_one.at[h, pl.ds(0, len(peers))]
        pltpu.make_async_copy(part, part, one_sem.at[1, h]).wait()
        goal = index // unit * rows + me * tile + unit * h + inner
        mix = (same & (first <= goal) & (goal < last)).astype(jnp.float32).astype(jnp.bfloat16)
        got = pieces(recv_one[h].reshape(span, width))
        send_two[h] = select(mix, got).reshape(shards, unit, width)
        for peer in early:
            pltpu.make_async_remote_copy(
                send_two.at[h, peer], packed_ref.at[me, pl.ds(unit * h, unit)], two_sem.at[0, h], two_sem.at[1, h],
                device_id={"shard": peer}, device_id_type=MESH,
            ).start()
        packed_ref[me, unit * h : unit * (h + 1)] = send_two[h, me]
    for h in range(CHUNKS):
        for peer in late:
            pltpu.make_async_remote_copy(
                send_two.at[h, peer], packed_ref.at[me, pl.ds(unit * h, unit)], two_sem.at[0, h], two_sem.at[1, h],
                device_id={"shard": peer}, device_id_type=MESH,
            ).start()
    filled_ref[...] = jnp.clip((me + 1) * rows - start, 0, rows)
    for h in range(CHUNKS):
        part = packed_ref.at[pl.ds(0, len(peers)), pl.ds(unit * h, unit)]
        pltpu.make_async_copy(part, part, two_sem.at[1, h]).wait()
    for h in range(CHUNKS):
        part = recv_one.at[h, pl.ds(0, len(peers))]
        pltpu.make_async_copy(part, part, one_sem.at[0, h]).wait()
        pltpu.make_async_copy(part, part, two_sem.at[0, h]).wait()
    pltpu.make_async_copy(line_part, line_part, line_sem.at[0]).wait()
    pltpu.make_async_copy(plane_part, plane_part, plane_sem.at[0]).wait()
    pltpu.make_async_copy(three, three, mask_sem.at[0]).wait()


def deliver(packed_ref, filled_ref, packed_out, stats_out, stats_buf, sem):
    shards, tile, width = packed_ref.shape
    rows = shards * tile
    leave = pltpu.make_async_copy(packed_ref, packed_out, sem.at[0])
    leave.start()
    filled = filled_ref[...]
    scale = jnp.maximum(filled.astype(jnp.float32), 1.0)
    slot = iota((shards, tile, width), 0) * tile + iota((shards, tile, width), 1)
    row_live = slot >= (rows - filled)[:, None]
    packed = packed_ref[...]
    total = jnp.sum(jnp.sum(packed, axis=0), axis=0, keepdims=True)
    low = jnp.min(jnp.min(jnp.where(row_live, packed, jnp.inf), axis=0), axis=0, keepdims=True)
    high = jnp.max(jnp.max(jnp.where(row_live, packed, -jnp.inf), axis=0), axis=0, keepdims=True)
    mean = total / scale
    away = packed - mean[None]
    spread = jnp.where(row_live, away * away, 0.0)
    variance = jnp.sum(jnp.sum(spread, axis=0), axis=0, keepdims=True) / scale
    low = jnp.where(filled > 0, low, 0.0)
    high = jnp.where(filled > 0, high, 0.0)
    for place, stat in enumerate((mean, variance, low, high)):
        stats_buf[place] = stat
    stats = pltpu.make_async_copy(stats_buf, stats_out, sem.at[1])
    stats.start()
    leave.wait()
    stats.wait()


def on_device(shards, groups, values, keep_mask, row_counts):
    rows, width = values.shape
    unit = rows // shards // CHUNKS
    blocks = pltpu.VMEM((CHUNKS, shards, unit, width), jnp.float32)
    packed, filled = pl.pallas_call(
        kernel,
        out_shape=(
            jax.ShapeDtypeStruct((shards, rows // shards, width), jnp.float32),
            jax.ShapeDtypeStruct((1, width), jnp.int32),
        ),
        in_specs=[pl.BlockSpec(memory_space=pltpu.HBM)] * 3,
        out_specs=(pl.BlockSpec(memory_space=pltpu.VMEM),) * 2,
        scratch_shapes=[
            pltpu.VMEM((rows, width), jnp.float32),
            pltpu.VMEM((1, width), jnp.int32),
            pltpu.VMEM((groups, 1, width), jnp.int32),
            pltpu.SMEM((1,), jnp.int32),
            pltpu.VMEM((1, width), jnp.int32),
            pltpu.VMEM((SIZES[0], 1, width), jnp.int32),
            pltpu.VMEM((1, width), jnp.int32),
            pltpu.VMEM((SIZES[1] * SIZES[2] * groups, 1, width), jnp.int32),
            blocks,
            blocks,
            blocks,
            pltpu.SemaphoreType.DMA((3,)),
            pltpu.SemaphoreType.DMA((2,)),
            pltpu.SemaphoreType.DMA((2,)),
            pltpu.SemaphoreType.DMA((2,)),
            pltpu.SemaphoreType.DMA((2, CHUNKS)),
            pltpu.SemaphoreType.DMA((2, CHUNKS)),
        ],
        name="compact",
        compiler_params=pltpu.CompilerParams(collective_id=0, has_side_effects=True, vmem_limit_bytes=8 * 1024 * 1024),
    )(
        pltpu.with_memory_space_constraint(values, pltpu.HBM),
        pltpu.with_memory_space_constraint(keep_mask.reshape(1, width), pltpu.HBM),
        row_counts,
    )
    packed, stats = pl.pallas_call(
        deliver,
        out_shape=(
            jax.ShapeDtypeStruct((shards, rows // shards, width), jnp.float32),
            jax.ShapeDtypeStruct((4, 1, width), jnp.float32),
        ),
        in_specs=[pl.BlockSpec(memory_space=pltpu.VMEM)] * 2,
        out_specs=(pl.BlockSpec(memory_space=pltpu.HBM),) * 2,
        scratch_shapes=[pltpu.VMEM((4, 1, width), jnp.float32), pltpu.SemaphoreType.DMA((2,))],
        name="deliver",
        compiler_params=pltpu.CompilerParams(vmem_limit_bytes=1024 * 1024),
    )(packed, filled)
    return packed.reshape(rows, width), stats


def solution(mesh):
    in_specs = (P("shard", "col"), P(("shard", "col")), P("shard"))
    out_specs = (P("shard", "col"), P(None, "shard", "col"))
    body = functools.partial(on_device, mesh.shape["shard"], mesh.shape["col"])
    return jax.shard_map(body, mesh=mesh, in_specs=in_specs, out_specs=out_specs, check_vma=False)
```

```python
import functools

import jax
import jax.numpy as jnp
from jax import lax
from jax.experimental import pallas as pl
from jax.experimental.pallas import tpu as pltpu
from jax.sharding import PartitionSpec as P

MESH = pl.DeviceIdType.MESH
CHUNKS = 4
SIZES = (8, 4, 2)


def hops(step):
    return sum(min(d, n - d) for d, n in zip(step[:2], SIZES[:2]))


STEPS = sorted(
    [(z, y, c) for z in range(8) for y in range(4) for c in range(2)][1:],
    key=lambda step: (-hops(step), (step[0] * 5 + step[1] * 3 + step[2] * 7) % 11, step),
)


PLANE = sorted(
    [(y, c, x) for y in range(4) for c in range(2) for x in range(4)][1:],
    key=lambda step: (-min(step[0], 4 - step[0]) - min(step[2], 4 - step[2]), step),
)


def iota(shape, dim):
    return lax.broadcasted_iota(jnp.int32, shape, dim)


def pieces(x):
    high = x.astype(jnp.bfloat16)
    rest = x - high.astype(jnp.float32)
    mid = rest.astype(jnp.bfloat16)
    low = (rest - mid.astype(jnp.float32)).astype(jnp.bfloat16)
    return jnp.concatenate([high, mid, low], axis=1)


def select(choice, parts):
    width = parts.shape[1] // 3
    out = jnp.dot(choice, parts, preferred_element_type=jnp.float32)
    return (out[:, :width] + out[:, width : 2 * width]) + out[:, 2 * width :]


def kernel(
    values_ref,
    mask_ref,
    counts_ref,
    packed_ref,
    filled_ref,
    values_buf,
    mask_own,
    mask_buf,
    counts_buf,
    kept_own,
    line_buf,
    line_own,
    plane_buf,
    send_one,
    recv_one,
    send_two,
    local_sem,
    mask_sem,
    line_sem,
    plane_sem,
    one_sem,
    two_sem,
):
    rows, width = values_buf.shape
    shards = send_one.shape[1]
    groups = mask_buf.shape[0]
    depth, breadth = SIZES[0], SIZES[1] * SIZES[2]
    unit = send_one.shape[2]
    span = shards * unit
    tile = rows // shards
    me = lax.axis_index("shard")
    col = lax.axis_index("col")

    load_mask = pltpu.make_async_copy(mask_ref, mask_own, local_sem.at[0])
    load_counts = pltpu.make_async_copy(counts_ref, counts_buf, local_sem.at[1])
    load_values = pltpu.make_async_copy(values_ref, values_buf, local_sem.at[2])
    load_mask.start()
    load_counts.start()
    load_values.start()

    z, y, c = me // 8, lax.rem(me // 2, 4), lax.rem(me, 2)
    cols = [lax.rem(col + d, 4) for d in (2, 1, 3)]
    lines = [lax.rem(z + dz, 8) * 8 + lax.rem(me, 8) for dz in (4, 3, 5, 2, 6, 1, 7)]
    planes = [
        {"shard": z * 8 + lax.rem(y + dy, 4) * 2 + lax.rem(c + dc, 2), "col": lax.rem(col + dx, 4)}
        for dy, dc, dx in PLANE
    ]

    barrier = pltpu.get_barrier_semaphore()
    for peer in lines:
        pl.semaphore_signal(barrier, inc=1, device_id={"shard": peer}, device_id_type=MESH)
    for peer in planes:
        pl.semaphore_signal(barrier, inc=1, device_id=peer, device_id_type=MESH)
    load_mask.wait()
    load_counts.wait()
    present = counts_buf[0]
    mine = (mask_own[...] == 1) & (col * width + iota((1, width), 1) < present)
    kept = jnp.sum(jnp.where(mine, 1, 0), axis=1, keepdims=True)
    kept_own[...] = jnp.broadcast_to(kept, (1, width))
    pl.semaphore_wait(barrier, len(lines) + len(planes))

    for peer in lines:
        pltpu.make_async_remote_copy(
            kept_own, line_buf.at[z], line_sem.at[0], line_sem.at[1],
            device_id={"shard": peer}, device_id_type=MESH,
        ).start()
    line_buf[z] = kept_own[...]
    mask_buf[col] = mask_own[...]
    line_part = line_buf.at[pl.ds(0, len(lines))]
    pltpu.make_async_copy(line_part, line_part, line_sem.at[1]).wait()
    level = iota((1, width), 1) // (width // depth)
    line = line_buf[0]
    for k in range(1, depth):
        line = jnp.where(level == k, line_buf[k], line)
    line_own[...] = line
    place_in_plane = lax.rem(me, breadth) * groups + col
    for peer in planes:
        pltpu.make_async_remote_copy(
            line_own, plane_buf.at[place_in_plane], plane_sem.at[0], plane_sem.at[1],
            device_id=peer, device_id_type=MESH,
        ).start()
    for peer in cols:
        pltpu.make_async_remote_copy(
            mask_own, mask_buf.at[col], mask_sem.at[0], mask_sem.at[1],
            device_id={"col": peer}, device_id_type=MESH,
        ).start()
    plane_buf[place_in_plane] = line_own[...]

    peers = [
        lax.rem(z + dz, 8) * 8 + lax.rem(y + dy, 4) * 2 + lax.rem(c + dc, 2)
        for dz, dy, dc in STEPS
    ]
    near = [z * 8 + lax.rem(y + dy, 4) * 2 + lax.rem(c + dc, 2) for dy, dc in ((2, 1), (2, 0), (1, 1), (3, 1), (1, 0), (3, 0), (0, 1))]
    climb = [
        (step - 1 + (step + 7 - z) // 8) * 8 + row * 2 + core
        for step in range(1, 8)
        for row in (0, 1, 3, 2)
        for core in (0, 1)
    ]
    early, late = near + climb[: 32], climb[32 :]

    load_values.wait()
    parts = pieces(values_buf[...])
    three = mask_buf.at[pl.ds(0, len(cols))]
    pltpu.make_async_copy(three, three, mask_sem.at[1]).wait()
    mask = jnp.concatenate([mask_buf[g] for g in range(groups)], axis=0)
    row = iota((groups, width), 0) * width + iota((groups, width), 1)
    live = (mask == 1) & (row < present)
    live_part = jnp.where(live, 1.0, 0.0).astype(jnp.bfloat16)
    ahead = (iota((width, width), 0) < iota((width, width), 1)).astype(jnp.float32).astype(jnp.bfloat16)
    inside = jnp.dot(live_part, ahead, preferred_element_type=jnp.float32)
    ones = jnp.ones((width, width), jnp.bfloat16)
    whole = jnp.dot(live_part, ones, preferred_element_type=jnp.float32)
    base = [jnp.zeros((1, width), jnp.float32)]
    for g in range(groups - 1):
        base.append(base[-1] + whole[g : g + 1])
    rank = (inside + jnp.concatenate(base, axis=0)).astype(jnp.int32)
    plane_part = plane_buf.at[pl.ds(0, len(planes))]
    pltpu.make_async_copy(plane_part, plane_part, plane_sem.at[1]).wait()

    plane = [
        sum(plane_buf[b * groups + g] for g in range(1, groups)) + plane_buf[b * groups] for b in range(breadth)
    ]
    plane = jnp.concatenate(plane, axis=0)
    every = jnp.concatenate(
        [
            jnp.broadcast_to(plane[:, k * (width // depth) : k * (width // depth) + 1], (breadth, width))
            for k in range(depth)
        ],
        axis=0,
    )
    shard = iota((shards, width), 0)
    mine = shards * rows - jnp.sum(jnp.where(shard >= me, every, 0), axis=0, keepdims=True)
    start = shards * rows - jnp.sum(every, axis=0, keepdims=True)
    target = mine + rank
    place = jnp.where(live, target - target // rows * rows, rows)

    index = iota((span, 1), 0)
    for h in range(CHUNKS):
        slot = index // unit * tile + unit * h + lax.rem(index, unit)
        choice = jnp.concatenate(
            [(slot == place[g : g + 1]).astype(jnp.float32).astype(jnp.bfloat16) for g in range(groups)], axis=1
        )
        send_one[h] = select(choice, parts).reshape(shards, unit, width)
        for peer in peers:
            pltpu.make_async_remote_copy(
                send_one.at[h, peer], recv_one.at[h, me], one_sem.at[0, h], one_sem.at[1, h],
                device_id={"shard": peer}, device_id_type=MESH,
            ).start()
        recv_one[h, me] = send_one[h, me]

    wide = jnp.concatenate([every] * max(1, span // width), axis=1)[:, :span]
    lane = iota((shards, span), 1) // unit
    source = iota((shards, span), 0)
    first = shards * rows - jnp.sum(jnp.where(source >= lane, wide, 0), axis=0, keepdims=True)
    last = shards * rows - jnp.sum(jnp.where(source > lane, wide, 0), axis=0, keepdims=True)
    inner = lax.rem(index, unit)
    same = inner == lax.rem(iota((1, span), 1), unit)
    for h in range(CHUNKS):
        part = recv_one.at[h, pl.ds(0, len(peers))]
        pltpu.make_async_copy(part, part, one_sem.at[1, h]).wait()
        goal = index // unit * rows + me * tile + unit * h + inner
        mix = (same & (first <= goal) & (goal < last)).astype(jnp.float32).astype(jnp.bfloat16)
        got = pieces(recv_one[h].reshape(span, width))
        send_two[h] = select(mix, got).reshape(shards, unit, width)
        for peer in early:
            pltpu.make_async_remote_copy(
                send_two.at[h, peer], packed_ref.at[me, pl.ds(unit * h, unit)], two_sem.at[0, h], two_sem.at[1, h],
                device_id={"shard": peer}, device_id_type=MESH,
            ).start()
        packed_ref[me, unit * h : unit * (h + 1)] = send_two[h, me]
    for h in range(CHUNKS):
        for peer in late:
            pltpu.make_async_remote_copy(
                send_two.at[h, peer], packed_ref.at[me, pl.ds(unit * h, unit)], two_sem.at[0, h], two_sem.at[1, h],
                device_id={"shard": peer}, device_id_type=MESH,
            ).start()
    filled_ref[...] = jnp.clip((me + 1) * rows - start, 0, rows)
    for h in range(CHUNKS):
        part = packed_ref.at[pl.ds(0, len(peers)), pl.ds(unit * h, unit)]
        pltpu.make_async_copy(part, part, two_sem.at[1, h]).wait()
    for h in range(CHUNKS):
        part = recv_one.at[h, pl.ds(0, len(peers))]
        pltpu.make_async_copy(part, part, one_sem.at[0, h]).wait()
        pltpu.make_async_copy(part, part, two_sem.at[0, h]).wait()
    pltpu.make_async_copy(line_part, line_part, line_sem.at[0]).wait()
    pltpu.make_async_copy(plane_part, plane_part, plane_sem.at[0]).wait()
    pltpu.make_async_copy(three, three, mask_sem.at[0]).wait()


def deliver(packed_ref, filled_ref, packed_out, stats_out, stats_buf, sem):
    shards, tile, width = packed_ref.shape
    rows = shards * tile
    leave = pltpu.make_async_copy(packed_ref, packed_out, sem.at[0])
    leave.start()
    filled = filled_ref[...]
    scale = jnp.maximum(filled.astype(jnp.float32), 1.0)
    slot = iota((shards, tile, width), 0) * tile + iota((shards, tile, width), 1)
    row_live = slot >= (rows - filled)[:, None]
    packed = packed_ref[...]
    total = jnp.sum(jnp.sum(packed, axis=0), axis=0, keepdims=True)
    low = jnp.min(jnp.min(jnp.where(row_live, packed, jnp.inf), axis=0), axis=0, keepdims=True)
    high = jnp.max(jnp.max(jnp.where(row_live, packed, -jnp.inf), axis=0), axis=0, keepdims=True)
    mean = total / scale
    away = packed - mean[None]
    spread = jnp.where(row_live, away * away, 0.0)
    variance = jnp.sum(jnp.sum(spread, axis=0), axis=0, keepdims=True) / scale
    low = jnp.where(filled > 0, low, 0.0)
    high = jnp.where(filled > 0, high, 0.0)
    for place, stat in enumerate((mean, variance, low, high)):
        stats_buf[place] = stat
    stats = pltpu.make_async_copy(stats_buf, stats_out, sem.at[1])
    stats.start()
    leave.wait()
    stats.wait()


def on_device(shards, groups, values, keep_mask, row_counts):
    rows, width = values.shape
    unit = rows // shards // CHUNKS
    blocks = pltpu.VMEM((CHUNKS, shards, unit, width), jnp.float32)
    packed, filled = pl.pallas_call(
        kernel,
        out_shape=(
            jax.ShapeDtypeStruct((shards, rows // shards, width), jnp.float32),
            jax.ShapeDtypeStruct((1, width), jnp.int32),
        ),
        in_specs=[pl.BlockSpec(memory_space=pltpu.HBM)] * 3,
        out_specs=(pl.BlockSpec(memory_space=pltpu.VMEM),) * 2,
        scratch_shapes=[
            pltpu.VMEM((rows, width), jnp.float32),
            pltpu.VMEM((1, width), jnp.int32),
            pltpu.VMEM((groups, 1, width), jnp.int32),
            pltpu.SMEM((1,), jnp.int32),
            pltpu.VMEM((1, width), jnp.int32),
            pltpu.VMEM((SIZES[0], 1, width), jnp.int32),
            pltpu.VMEM((1, width), jnp.int32),
            pltpu.VMEM((SIZES[1] * SIZES[2] * groups, 1, width), jnp.int32),
            blocks,
            blocks,
            blocks,
            pltpu.SemaphoreType.DMA((3,)),
            pltpu.SemaphoreType.DMA((2,)),
            pltpu.SemaphoreType.DMA((2,)),
            pltpu.SemaphoreType.DMA((2,)),
            pltpu.SemaphoreType.DMA((2, CHUNKS)),
            pltpu.SemaphoreType.DMA((2, CHUNKS)),
        ],
        name="compact",
        compiler_params=pltpu.CompilerParams(collective_id=0, has_side_effects=True, vmem_limit_bytes=8 * 1024 * 1024),
    )(
        pltpu.with_memory_space_constraint(values, pltpu.HBM),
        pltpu.with_memory_space_constraint(keep_mask.reshape(1, width), pltpu.HBM),
        row_counts,
    )
    packed, stats = pl.pallas_call(
        deliver,
        out_shape=(
            jax.ShapeDtypeStruct((shards, rows // shards, width), jnp.float32),
            jax.ShapeDtypeStruct((4, 1, width), jnp.float32),
        ),
        in_specs=[pl.BlockSpec(memory_space=pltpu.VMEM)] * 2,
        out_specs=(pl.BlockSpec(memory_space=pltpu.HBM),) * 2,
        scratch_shapes=[pltpu.VMEM((4, 1, width), jnp.float32), pltpu.SemaphoreType.DMA((2,))],
        name="deliver",
        compiler_params=pltpu.CompilerParams(vmem_limit_bytes=1024 * 1024),
    )(packed, filled)
    return packed.reshape(rows, width), stats


def solution(mesh):
    in_specs = (P("shard", "col"), P(("shard", "col")), P("shard"))
    out_specs = (P("shard", "col"), P(None, "shard", "col"))
    body = functools.partial(on_device, mesh.shape["shard"], mesh.shape["col"])
    return jax.shard_map(body, mesh=mesh, in_specs=in_specs, out_specs=out_specs, check_vma=False)
```
